32 devices in a mesh: rep: 2 (over x), blk: 16 (over z, y, core).
Axes of the slice: x: 2, y: 2, z: 4, core: 2. Of those that a mesh axis runs over, the one named last changes fastest.
Arguments:
- positions: float32 [3, 8192], P(None, ('rep', 'blk')), parts along dimension 1, may hold values from 0 to 64
- forces: float32 [6, 3, 8192], P(None, None, ('rep', 'blk')), parts along dimension 2, may hold values from -6 to 6
- random_kicks: float32 [6, 3, 8192], P(None, None, ('rep', 'blk')), parts along dimension 2, may hold values from -4 to 4
- history_velocity: float32 [128, 3, 8192], P(None, None, ('rep', 'blk')), parts along dimension 2, may hold values from -6 to 6
- history_offset: float32 [128, 3, 8192], P(None, None, ('rep', 'blk')), parts along dimension 2, may hold values from -8 to 8
- lag_index: int32 [4096], P(('rep', 'blk')), parts along dimension 0, may hold values from 0 to 127
Outputs:
- final_positions: float32 [3, 8192], P(None, ('rep', 'blk')), parts along dimension 1
- velocity: float32 [3, 8192], P(None, ('rep', 'blk')), parts along dimension 1
- statistics: float32 [2, 4096], P(None, ('rep', 'blk')), parts along dimension 1
The draws below stay inside these ranges and needn't reach their ends.
There are 2 independent parts, one for each index of `rep`. The reference program is written for one: setup_inputs(seed, part) draws one part's arguments, and reference() takes and returns one part's arrays. A program takes and returns all parts, laid end to end along the dimension named above; each array names one. Nothing has to cross between parts.
All inputs are finite; a program needn't handle non-finite values.
Results may differ from the reference program's by a relative error of at most 0.0003.
Values sent between devices are 32-bit elements; how exact they have to be, the bound alone decides.
A program may use at most 64 MiB of HBM per device.

```python
import math
import jax
import jax.numpy as jnp
from jax import lax

STEPS = 6
HIST = 128
SPHERES = 4096
NLAG = 2048


def plant(result, own_key, least, high):
    longest = result.shape.index(max(result.shape))
    spots = []
    for shift in (0, 1):
        where = [jax.random.randint(jax.random.fold_in(own_key, axis), (), 0, length) for axis, length in enumerate(result.shape)]
        where[longest] = (where[longest] + shift) % result.shape[longest]
        spots.append(tuple(where))
    return result.at[spots[0]].set(least).at[spots[1]].set(high)


def steps_of(key, dims, pieces, least, high):
    factor_of, own = 1.0, jax.random.fold_in(key, 6)
    for axis_at, parts in pieces:
        draws = jnp.exp(jax.random.uniform(jax.random.fold_in(own, axis_at), (parts,), jnp.float32, least / len(pieces), high / len(pieces)))
        factor_of = factor_of * jnp.repeat(draws, dims[axis_at] // parts).reshape([-1 if axis == axis_at else 1 for axis in range(len(dims))])
    return factor_of


def noise(own_key, shape, spread, most, pieces=(), kind=jnp.bfloat16):
    array = spread * jax.random.normal(own_key, shape, jnp.float32)
    if pieces:
        array = array * steps_of(own_key, shape, pieces, -0.22, 0.18)
    return jnp.clip(array, -most, most).astype(kind)


def setup_inputs(seed: int = 0, part: int = 0) -> dict:
    arg_keys = jax.random.split(jax.random.key(seed), 7)
    own_keys = jax.random.split(jax.random.fold_in(arg_keys[6], part), 7)
    positions = jnp.clip(64.0 * jax.random.uniform(own_keys[0], (3, SPHERES), jnp.float32) ** steps_of(own_keys[0], (3, SPHERES), ((1, 16),), -0.2, 0.2), 0.0, 64.0)
    forces = noise(own_keys[1], (STEPS, 3, SPHERES), 1.0, 6.0, ((2, 16),), jnp.float32)
    random_kicks = noise(own_keys[2], (STEPS, 3, SPHERES), 0.3, 4.0, ((2, 16),), jnp.float32)
    history_velocity = noise(own_keys[3], (HIST, 3, SPHERES), 1.0, 6.0, ((2, 16),), jnp.float32)
    history_offset = noise(own_keys[4], (HIST, 3, SPHERES), 2.0, 8.0, ((2, 16),), jnp.float32)
    lag_index = plant(jax.random.randint(own_keys[5], (NLAG,), 0, HIST), jax.random.fold_in(own_keys[5], 1), 0, HIST - 1).astype(jnp.int32)
    return dict(positions=positions, forces=forces, random_kicks=random_kicks, history_velocity=history_velocity, history_offset=history_offset, lag_index=lag_index)


time_step = 0.05

def pair_velocity(targets, sources, loads):
    separation = targets[:, None, :] - sources[:, :, None]
    dist_sq = lax.optimization_barrier(jnp.sum(separation * separation, axis=0))
    dist_safe = jnp.where(dist_sq > 0.0, dist_sq, 1.0)
    inv_dist = lax.rsqrt(dist_safe)
    distance = dist_sq * inv_dist
    inv_sq = 1.0 / dist_safe
    far_mask = distance >= 2.0
    coef_iso = jnp.where(far_mask, 0.75 * inv_dist * (1.0 + 2.0 / 3.0 * inv_sq), 1.0 - 9.0 / 32.0 * distance)
    coef_dir = jnp.where(far_mask, 0.75 * inv_dist * (1.0 - 2.0 * inv_sq) * inv_sq, 3.0 / 32.0 * inv_dist)
    projection = lax.optimization_barrier(jnp.sum(separation * loads[:, :, None], axis=0))
    return lax.optimization_barrier(jnp.sum(coef_iso[None] * loads[:, :, None] + (coef_dir * projection)[None] * separation, axis=1))

def velocities(places, loads):
    row_count = math.gcd(SPHERES, 512)
    block_count = SPHERES // row_count
    source_blocks = places.reshape(3, block_count, row_count).transpose(1, 0, 2)
    load_blocks = loads.reshape(3, block_count, row_count).transpose(1, 0, 2)

    def accumulate(running, source_block):
        return (running + pair_velocity(places, source_block[0], source_block[1]), None)
    running, unused = lax.scan(accumulate, jnp.zeros((3, SPHERES), jnp.float32), (source_blocks, load_blocks))
    return running

def reference(positions, forces, random_kicks, history_velocity, history_offset, lag_index):
    places = positions
    velocity = jnp.zeros_like(positions)
    for step_index in range(STEPS):
        velocity = velocities(places, forces[step_index])
        places = places + time_step * velocity + random_kicks[step_index]
    velocity_dot = lax.optimization_barrier(jnp.sum(velocity[None] * history_velocity, axis=(1, 2)))
    moved = places[None] - positions[None] - history_offset
    square_disp = lax.optimization_barrier(jnp.sum(moved * moved, axis=(1, 2)))
    statistics = jnp.stack([velocity_dot[lag_index], square_disp[lag_index]]) / jnp.float32(SPHERES)
    return (places, velocity, statistics)
```

```python
import functools

import jax
import jax.numpy as jnp
from jax import lax
from jax.experimental import pallas as pl
from jax.experimental.pallas import tpu as pltpu
from jax.sharding import PartitionSpec as P

TIME_STEP = 0.05
LANES = 128
ROWS = 64


def pieces(value):
    high = value.astype(jnp.bfloat16)
    rest = value - high.astype(jnp.float32)
    mid = rest.astype(jnp.bfloat16)
    low = (rest - mid.astype(jnp.float32)).astype(jnp.bfloat16)
    return (high, mid, low)


def lane_sums(value):
    ones = jnp.ones((8, value.shape[1]), jnp.bfloat16)
    total = None
    for piece in pieces(value):
        term = lax.dot_general(
            ones, piece, (((1,), (1,)), ((), ())), preferred_element_type=jnp.float32
        )
        total = term if total is None else total + term
    return total


def kernel(
    n, steps, pos_ref, force_ref, kick_ref, hv_ref, ho_ref, lag_ref,
    out_pos, out_vel, out_stat,
    places, loads, cols, acc, hv, ho, table, tables,
    send_sem, recv_sem, fsend_sem, frecv_sem, tsend_sem, trecv_sem, hist_sem,
):
    me = lax.axis_index("blk")
    width = pos_ref.shape[1]
    tiles = width // LANES
    frames = hv_ref.shape[1]

    def partner(index):
        far = (index + 1) // 2
        sign = 2 * (index % 2) - 1
        return lax.rem(me + far * sign + n, n)

    def other(index):
        far = (index + 1) // 2
        sign = 2 * (index % 2) - 1
        return lax.rem(me - far * sign + n, n)

    get_hv = pltpu.make_async_copy(hv_ref, hv, hist_sem.at[0])
    get_ho = pltpu.make_async_copy(ho_ref, ho, hist_sem.at[1])
    get_hv.start()
    get_ho.start()

    barrier = pltpu.get_barrier_semaphore()

    @pl.loop(1, n)
    def _(index):
        pl.semaphore_signal(barrier, inc=1, device_id={"blk": partner(index)})

    def place_copy(step, owner, target):
        return pltpu.make_async_remote_copy(
            src_ref=places.at[step, me],
            dst_ref=places.at[step, owner],
            send_sem=send_sem.at[target],
            recv_sem=recv_sem.at[lax.rem(step, 2), owner],
            device_id={"blk": target},
        )

    def load_copy(owner, target):
        return pltpu.make_async_remote_copy(
            src_ref=loads.at[me],
            dst_ref=loads.at[owner],
            send_sem=fsend_sem.at[target],
            recv_sem=frecv_sem.at[owner],
            device_id={"blk": target},
        )

    def table_copy(owner, target):
        return pltpu.make_async_remote_copy(
            src_ref=table,
            dst_ref=tables.at[owner],
            send_sem=tsend_sem.at[target],
            recv_sem=trecv_sem.at[owner],
            device_id={"blk": target},
        )

    loads[me] = force_ref[...]
    places[0, me] = pos_ref[...] * 0.5
    pl.semaphore_wait(barrier, n - 1)

    @pl.loop(1, n)
    def _(index):
        place_copy(0, me, partner(index)).start()
        load_copy(me, partner(index)).start()

    @pl.loop(0, steps)
    def _(step):
        mine = places[step, me]
        padded = jnp.concatenate([mine, jnp.zeros((5, width), jnp.float32)], axis=0)
        turned = jnp.transpose(padded)
        for comp in range(3):
            cols[comp] = jnp.broadcast_to(turned[:, comp : comp + 1], (width, LANES))
            acc[comp] = jnp.zeros((width, LANES), jnp.float32)

        @pl.loop(0, n)
        def _(index):
            source = partner(index)

            @pl.when(index > 0)
            def _():
                place_copy(step, source, source).wait_recv()

            @pl.when(jnp.logical_and(index > 0, step == 0))
            def _():
                load_copy(source, source).wait_recv()

            @pl.loop(0, width // ROWS)
            def _(chunk):
                rows = pl.ds(pl.multiple_of(chunk * ROWS, ROWS), ROWS)
                target = [cols[comp, rows, :] for comp in range(3)]
                sums = [acc[comp, rows, :] for comp in range(3)]
                for tile in range(tiles):
                    lanes = pl.ds(tile * LANES, LANES)
                    sep = [
                        target[comp] - places[step, source, pl.ds(comp, 1), lanes]
                        for comp in range(3)
                    ]
                    load = [
                        loads[source, step, pl.ds(comp, 1), lanes] for comp in range(3)
                    ]
                    dist_sq = sep[0] * sep[0] + sep[1] * sep[1] + sep[2] * sep[2]
                    dist_sq = jnp.maximum(dist_sq, 1e-30)
                    inv = lax.rsqrt(dist_sq)
                    cut = jnp.minimum(inv, 1.0)
                    cut_sq = cut * cut
                    near = jnp.maximum(1.0 - dist_sq * inv, 0.0)
                    iso = cut * (6.0 + cut_sq) + 9.0 * near
                    along = cut * cut_sq * (2.0 - cut_sq) + (inv - cut)
                    push = along * (
                        sep[0] * (3.0 * load[0])
                        + sep[1] * (3.0 * load[1])
                        + sep[2] * (3.0 * load[2])
                    )
                    for comp in range(3):
                        sums[comp] = sums[comp] + (iso * load[comp] + push * sep[comp])
                for comp in range(3):
                    acc[comp, rows, :] = sums[comp]

        vel = jnp.concatenate(
            [lane_sums(acc[comp])[0:1] for comp in range(3)], axis=0
        ) * (1.0 / 16.0)

        @pl.loop(1, n)
        def _(index):
            place_copy(step, me, partner(index)).wait_send()

        fresh = mine + (0.5 * TIME_STEP) * vel + 0.5 * kick_ref[step]
        out_vel[...] = vel

        @pl.when(step < steps - 1)
        def _():
            places[step + 1, me] = fresh

            @pl.loop(1, n)
            def _(index):
                place_copy(step + 1, me, partner(index)).start()

        @pl.when(step == steps - 1)
        def _():
            out_pos[...] = 2.0 * fresh

    @pl.loop(1, n)
    def _(index):
        load_copy(me, partner(index)).wait_send()

    get_hv.wait()
    get_ho.wait()
    vel = out_vel[...]
    moved = out_pos[...] - pos_ref[...]
    dot = jnp.zeros((frames, LANES), jnp.float32)
    square = jnp.zeros((frames, LANES), jnp.float32)
    for comp in range(3):
        for tile in range(tiles):
            lanes = slice(tile * LANES, (tile + 1) * LANES)
            dot = dot + vel[comp : comp + 1, lanes] * hv[comp, :, lanes]
            gap = moved[comp : comp + 1, lanes] - ho[comp, :, lanes]
            square = square + gap * gap
    table[...] = jnp.concatenate([lane_sums(dot)[0:1], lane_sums(square)[0:1]], axis=0)

    @pl.loop(1, n)
    def _(index):
        table_copy(me, partner(index)).start()

    onehot = (
        lax.broadcasted_iota(jnp.int32, (frames, lag_ref.shape[1]), 0) == lag_ref[...]
    ).astype(jnp.bfloat16)
    tables[me] = table[...]

    @pl.loop(1, n)
    def _(index):
        table_copy(partner(index), partner(index)).wait_recv()

    whole = tables[0]
    for index in range(1, n):
        whole = whole + tables[index]
    whole = jnp.concatenate([whole, jnp.zeros((6, frames), jnp.float32)], axis=0)
    stat = None
    for piece in pieces(whole):
        term = jnp.dot(piece, onehot, preferred_element_type=jnp.float32)
        stat = term if stat is None else stat + term
    out_stat[...] = stat[0:2] / jnp.float32(width * n)

    @pl.loop(1, n)
    def _(index):
        table_copy(me, partner(index)).wait_send()


def local(n, positions, forces, random_kicks, history_velocity, history_offset, lag_index):
    steps = forces.shape[0]
    width = positions.shape[1]
    frames = history_velocity.shape[0]
    lags = lag_index.shape[0]
    vmem = pl.BlockSpec(memory_space=pltpu.VMEM)
    hbm = pl.BlockSpec(memory_space=pl.ANY)
    return pl.pallas_call(
        functools.partial(kernel, n, steps),
        out_shape=(
            jax.ShapeDtypeStruct((3, width), jnp.float32),
            jax.ShapeDtypeStruct((3, width), jnp.float32),
            jax.ShapeDtypeStruct((2, lags), jnp.float32),
        ),
        in_specs=[vmem, vmem, vmem, hbm, hbm, vmem],
        out_specs=(vmem, vmem, vmem),
        scratch_shapes=[
            pltpu.VMEM((steps, n, 3, width), jnp.float32),
            pltpu.VMEM((n, steps, 3, width), jnp.float32),
            pltpu.VMEM((3, width, LANES), jnp.float32),
            pltpu.VMEM((3, width, LANES), jnp.float32),
            pltpu.VMEM((3, frames, width), jnp.float32),
            pltpu.VMEM((3, frames, width), jnp.float32),
            pltpu.VMEM((2, frames), jnp.float32),
            pltpu.VMEM((n, 2, frames), jnp.float32),
            pltpu.SemaphoreType.DMA((n,)),
            pltpu.SemaphoreType.DMA((2, n)),
            pltpu.SemaphoreType.DMA((n,)),
            pltpu.SemaphoreType.DMA((n,)),
            pltpu.SemaphoreType.DMA((n,)),
            pltpu.SemaphoreType.DMA((n,)),
            pltpu.SemaphoreType.DMA((2,)),
        ],
        compiler_params=pltpu.CompilerParams(collective_id=0, has_side_effects=True),
    )(
        positions,
        forces,
        random_kicks,
        history_velocity.transpose(1, 0, 2),
        history_offset.transpose(1, 0, 2),
        lag_index.reshape(1, lags),
    )


def solution(mesh):
    return jax.shard_map(
        functools.partial(local, mesh.shape["blk"]),
        mesh=mesh,
        in_specs=(
            P(None, ("rep", "blk")),
            P(None, None, ("rep", "blk")),
            P(None, None, ("rep", "blk")),
            P(None, None, ("rep", "blk")),
            P(None, None, ("rep", "blk")),
            P(("rep", "blk")),
        ),
        out_specs=(P(None, ("rep", "blk")), P(None, ("rep", "blk")), P(None, ("rep", "blk"))),
        check_vma=False,
    )
```

```python
import functools

import jax
import jax.numpy as jnp
from jax import lax
from jax.experimental import pallas as pl
from jax.experimental.pallas import tpu as pltpu
from jax.sharding import PartitionSpec as P

TIME_STEP = 0.05
LANES = 128
ROWS = 64


def pieces(value):
    high = value.astype(jnp.bfloat16)
    rest = value - high.astype(jnp.float32)
    mid = rest.astype(jnp.bfloat16)
    low = (rest - mid.astype(jnp.float32)).astype(jnp.bfloat16)
    return (high, mid, low)


def lane_sums(value):
    ones = jnp.ones((8, value.shape[1]), jnp.bfloat16)
    total = None
    for piece in pieces(value):
        term = lax.dot_general(
            ones, piece, (((1,), (1,)), ((), ())), preferred_element_type=jnp.float32
        )
        total = term if total is None else total + term
    return total


def kernel(
    n, steps, pos_ref, force_ref, kick_ref, hv_ref, ho_ref, lag_ref,
    out_pos, out_vel, out_stat,
    places, loads, cols, acc, hv, ho, table, tables,
    send_sem, recv_sem, pass_sem, fsend_sem, frecv_sem, tsend_sem, trecv_sem, hist_sem,
):
    me = lax.axis_index("blk")
    width = pos_ref.shape[1]
    tiles = width // LANES
    frames = hv_ref.shape[1]

    cores = 2 if n % 2 == 0 else 1
    chips = n // cores
    per = 2 if chips % 2 == 0 else 1
    planes = chips // per
    core, chip = me % cores, me // cores
    plane, seat = chip // per, chip % per
    edge = jnp.minimum(plane, planes - 1 - plane)
    low = plane < planes - 1 - plane
    twin = chip * cores + (core + 1) % cores

    def partner(index):
        return lax.rem(me + index, n)

    def chip_at(order):
        hop, sub = order // per, order % per
        far = jnp.where(hop <= 2 * edge, (hop + 1) // 2, hop - edge)
        ahead = jnp.where(hop <= 2 * edge, hop % 2 == 1, low)
        return (plane + jnp.where(ahead, far, -far)) * per + (seat + sub) % per

    def peer(order):
        return chip_at(order) * cores + core

    get_hv = pltpu.make_async_copy(hv_ref, hv, hist_sem.at[0])
    get_ho = pltpu.make_async_copy(ho_ref, ho, hist_sem.at[1])
    get_hv.start()
    get_ho.start()

    barrier = pltpu.get_barrier_semaphore()

    @pl.loop(1, n)
    def _(index):
        pl.semaphore_signal(barrier, inc=1, device_id={"blk": partner(index)})

    def place_copy(step, owner, target, sem):
        return pltpu.make_async_remote_copy(
            src_ref=places.at[step, owner],
            dst_ref=places.at[step, owner],
            send_sem=sem,
            recv_sem=recv_sem.at[lax.rem(step, 2), owner],
            device_id={"blk": target},
        )

    def load_copy(part, owner, target, sem):
        first, count = ((0, 1), (1, steps - 1))[part]
        return pltpu.make_async_remote_copy(
            src_ref=loads.at[owner, pl.ds(first, count)],
            dst_ref=loads.at[owner, pl.ds(first, count)],
            send_sem=sem,
            recv_sem=frecv_sem.at[part, owner],
            device_id={"blk": target},
        )

    def place_out(step, action):
        if cores == 2:
            getattr(place_copy(step, me, twin, send_sem.at[twin]), action)()

        @pl.loop(1, chips)
        def _(order):
            to = peer(order)
            getattr(place_copy(step, me, to, send_sem.at[to]), action)()

    def load_out(part, action):
        if cores == 2:
            getattr(load_copy(part, me, twin, fsend_sem.at[part, twin]), action)()

        @pl.loop(1, chips)
        def _(order):
            to = peer(order)
            getattr(load_copy(part, me, to, fsend_sem.at[part, to]), action)()

    def table_copy(owner, target):
        return pltpu.make_async_remote_copy(
            src_ref=table,
            dst_ref=tables.at[owner],
            send_sem=tsend_sem.at[target],
            recv_sem=trecv_sem.at[owner],
            device_id={"blk": target},
        )

    loads[me] = force_ref[...]
    places[0, me] = pos_ref[...] * 0.5
    pl.semaphore_wait(barrier, n - 1)

    place_out(0, "start")
    load_out(0, "start")
    if steps > 1:
        load_out(1, "start")

    @pl.loop(0, steps)
    def _(step):
        mine = places[step, me]
        padded = jnp.concatenate([mine, jnp.zeros((5, width), jnp.float32)], axis=0)
        turned = jnp.transpose(padded)
        for comp in range(3):
            cols[comp] = jnp.broadcast_to(turned[:, comp : comp + 1], (width, LANES))
            acc[comp] = jnp.zeros((width, LANES), jnp.float32)

        @pl.loop(0, n)
        def _(index):
            if cores == 2:
                direct = jnp.logical_or(
                    index == 0, jnp.logical_and(index % 2 == 1, index < n - 1)
                )
                order = jnp.where(
                    direct,
                    (index + 1) // 2,
                    jnp.where(index == n - 1, chips - 1, (index - 2) // 2),
                )
                side = jnp.where(direct, core, 1 - core)
                source = chip_at(order) * cores + side
                passing = jnp.logical_and(direct, index > 0)
            else:
                source = peer(index)
                passing = None

            @pl.when(index > 0)
            def _():
                place_copy(step, source, source, send_sem.at[source]).wait_recv()

            if passing is not None:

                @pl.when(passing)
                def _():
                    place_copy(step, source, twin, pass_sem.at[0, source]).start()

            for part in range(min(2, steps)):

                @pl.when(jnp.logical_and(index > 0, step == part))
                def _():
                    load_copy(part, source, source, fsend_sem.at[part, source]).wait_recv()

                if passing is not None:

                    @pl.when(jnp.logical_and(passing, step == part))
                    def _():
                        load_copy(part, source, twin, pass_sem.at[part + 1, source]).start()

            @pl.loop(0, width // ROWS)
            def _(chunk):
                rows = pl.ds(pl.multiple_of(chunk * ROWS, ROWS), ROWS)
                target = [cols[comp, rows, :] for comp in range(3)]
                sums = [acc[comp, rows, :] for comp in range(3)]
                for tile in range(tiles):
                    lanes = pl.ds(tile * LANES, LANES)
                    sep = [
                        target[comp] - places[step, source, pl.ds(comp, 1), lanes]
                        for comp in range(3)
                    ]
                    load = [
                        loads[source, step, pl.ds(comp, 1), lanes] for comp in range(3)
                    ]
                    dist_sq = sep[0] * sep[0] + sep[1] * sep[1] + sep[2] * sep[2]
                    dist_sq = jnp.maximum(dist_sq, 1e-30)
                    inv = lax.rsqrt(dist_sq)
                    cut = jnp.minimum(inv, 1.0)
                    cut_sq = cut * cut
                    near = jnp.maximum(1.0 - dist_sq * inv, 0.0)
                    iso = cut * (6.0 + cut_sq) + 9.0 * near
                    rest = 1.0 - cut_sq
                    along = inv - cut * (rest * rest)
                    push = along * (
                        sep[0] * (3.0 * load[0])
                        + sep[1] * (3.0 * load[1])
                        + sep[2] * (3.0 * load[2])
                    )
                    for comp in range(3):
                        sums[comp] = sums[comp] + (iso * load[comp] + push * sep[comp])
                for comp in range(3):
                    acc[comp, rows, :] = sums[comp]

        vel = jnp.concatenate(
            [lane_sums(acc[comp])[0:1] for comp in range(3)], axis=0
        ) * (1.0 / 16.0)

        place_out(step, "wait_send")
        if cores == 2:

            @pl.loop(1, chips)
            def _(order):
                source = peer(order)
                place_copy(step, source, twin, pass_sem.at[0, source]).wait_send()

        fresh = mine + (0.5 * TIME_STEP) * vel + 0.5 * kick_ref[step]
        out_vel[...] = vel

        @pl.when(step < steps - 1)
        def _():
            places[step + 1, me] = fresh

            place_out(step + 1, "start")

        @pl.when(step == steps - 1)
        def _():
            out_pos[...] = 2.0 * fresh

    for part in range(min(2, steps)):
        load_out(part, "wait_send")
        if cores == 2:

            @pl.loop(1, chips)
            def _(order):
                source = peer(order)
                load_copy(part, source, twin, pass_sem.at[part + 1, source]).wait_send()

    get_hv.wait()
    get_ho.wait()
    vel = out_vel[...]
    moved = out_pos[...] - pos_ref[...]
    dot = jnp.zeros((frames, LANES), jnp.float32)
    square = jnp.zeros((frames, LANES), jnp.float32)
    for comp in range(3):
        for tile in range(tiles):
            lanes = slice(tile * LANES, (tile + 1) * LANES)
            dot = dot + vel[comp : comp + 1, lanes] * hv[comp, :, lanes]
            gap = moved[comp : comp + 1, lanes] - ho[comp, :, lanes]
            square = square + gap * gap
    table[...] = jnp.concatenate([lane_sums(dot)[0:1], lane_sums(square)[0:1]], axis=0)

    @pl.loop(1, n)
    def _(index):
        table_copy(me, partner(index)).start()

    onehot = (
        lax.broadcasted_iota(jnp.int32, (frames, lag_ref.shape[1]), 0) == lag_ref[...]
    ).astype(jnp.bfloat16)
    tables[me] = table[...]

    @pl.loop(1, n)
    def _(index):
        table_copy(partner(index), partner(index)).wait_recv()

    whole = tables[0]
    for index in range(1, n):
        whole = whole + tables[index]
    whole = jnp.concatenate([whole, jnp.zeros((6, frames), jnp.float32)], axis=0)
    stat = None
    for piece in pieces(whole):
        term = jnp.dot(piece, onehot, preferred_element_type=jnp.float32)
        stat = term if stat is None else stat + term
    out_stat[...] = stat[0:2] / jnp.float32(width * n)

    @pl.loop(1, n)
    def _(index):
        table_copy(me, partner(index)).wait_send()


def local(n, positions, forces, random_kicks, history_velocity, history_offset, lag_index):
    steps = forces.shape[0]
    width = positions.shape[1]
    frames = history_velocity.shape[0]
    lags = lag_index.shape[0]
    vmem = pl.BlockSpec(memory_space=pltpu.VMEM)
    hbm = pl.BlockSpec(memory_space=pl.ANY)
    return pl.pallas_call(
        functools.partial(kernel, n, steps),
        out_shape=(
            jax.ShapeDtypeStruct((3, width), jnp.float32),
            jax.ShapeDtypeStruct((3, width), jnp.float32),
            jax.ShapeDtypeStruct((2, lags), jnp.float32),
        ),
        in_specs=[vmem, vmem, vmem, hbm, hbm, vmem],
        out_specs=(vmem, vmem, vmem),
        scratch_shapes=[
            pltpu.VMEM((steps, n, 3, width), jnp.float32),
            pltpu.VMEM((n, steps, 3, width), jnp.float32),
            pltpu.VMEM((3, width, LANES), jnp.float32),
            pltpu.VMEM((3, width, LANES), jnp.float32),
            pltpu.VMEM((3, frames, width), jnp.float32),
            pltpu.VMEM((3, frames, width), jnp.float32),
            pltpu.VMEM((2, frames), jnp.float32),
            pltpu.VMEM((n, 2, frames), jnp.float32),
            pltpu.SemaphoreType.DMA((n,)),
            pltpu.SemaphoreType.DMA((2, n)),
            pltpu.SemaphoreType.DMA((3, n)),
            pltpu.SemaphoreType.DMA((2, n)),
            pltpu.SemaphoreType.DMA((2, n)),
            pltpu.SemaphoreType.DMA((n,)),
            pltpu.SemaphoreType.DMA((n,)),
            pltpu.SemaphoreType.DMA((2,)),
        ],
        compiler_params=pltpu.CompilerParams(collective_id=0, has_side_effects=True),
    )(
        positions,
        forces,
        random_kicks,
        history_velocity.transpose(1, 0, 2),
        history_offset.transpose(1, 0, 2),
        lag_index.reshape(1, lags),
    )


def solution(mesh):
    return jax.shard_map(
        functools.partial(local, mesh.shape["blk"]),
        mesh=mesh,
        in_specs=(
            P(None, ("rep", "blk")),
            P(None, None, ("rep", "blk")),
            P(None, None, ("rep", "blk")),
            P(None, None, ("rep", "blk")),
            P(None, None, ("rep", "blk")),
            P(("rep", "blk")),
        ),
        out_specs=(P(None, ("rep", "blk")), P(None, ("rep", "blk")), P(None, ("rep", "blk"))),
        check_vma=False,
    )
```

```python
import functools

import jax
import jax.numpy as jnp
from jax import lax
from jax.experimental import pallas as pl
from jax.experimental.pallas import tpu as pltpu
from jax.sharding import PartitionSpec as P

TIME_STEP = 0.05
LANES = 128
ROWS = 128


def pieces(value):
    high = value.astype(jnp.bfloat16)
    rest = value - high.astype(jnp.float32)
    mid = rest.astype(jnp.bfloat16)
    low = (rest - mid.astype(jnp.float32)).astype(jnp.bfloat16)
    return (high, mid, low)


def lane_sums(value):
    ones = jnp.ones((8, value.shape[1]), jnp.bfloat16)
    total = None
    for piece in pieces(value):
        term = lax.dot_general(
            ones, piece, (((1,), (1,)), ((), ())), preferred_element_type=jnp.float32
        )
        total = term if total is None else total + term
    return total


def kernel(
    n, steps, pos_ref, force_ref, kick_ref, hv_ref, ho_ref, lag_ref,
    out_pos, out_vel, out_stat,
    places, loads, cols, acc, hv, ho, table, tables,
    send_sem, recv_sem, pass_sem, fsend_sem, frecv_sem, tsend_sem, trecv_sem, hist_sem,
):
    me = lax.axis_index("blk")
    width = pos_ref.shape[1]
    tiles = width // LANES
    frames = hv_ref.shape[1]

    cores = 2 if n % 2 == 0 else 1
    chips = n // cores
    per = 2 if chips % 2 == 0 else 1
    planes = chips // per
    core, chip = me % cores, me // cores
    plane, seat = chip // per, chip % per
    edge = jnp.minimum(plane, planes - 1 - plane)
    low = plane < planes - 1 - plane
    twin = chip * cores + (core + 1) % cores

    def partner(index):
        return lax.rem(me + index, n)

    def chip_at(order):
        hop, sub = order // per, order % per
        far = jnp.where(hop <= 2 * edge, (hop + 1) // 2, hop - edge)
        ahead = jnp.where(hop <= 2 * edge, hop % 2 == 1, low)
        return (plane + jnp.where(ahead, far, -far)) * per + (seat + sub) % per

    def peer(order):
        return chip_at(order) * cores + core

    get_hv = pltpu.make_async_copy(hv_ref, hv, hist_sem.at[0])
    get_ho = pltpu.make_async_copy(ho_ref, ho, hist_sem.at[1])
    get_hv.start()
    get_ho.start()

    barrier = pltpu.get_barrier_semaphore()

    @pl.loop(1, n)
    def _(index):
        pl.semaphore_signal(barrier, inc=1, device_id={"blk": partner(index)})

    def place_copy(step, owner, target, sem):
        return pltpu.make_async_remote_copy(
            src_ref=places.at[step, owner],
            dst_ref=places.at[step, owner],
            send_sem=sem,
            recv_sem=recv_sem.at[lax.rem(step, 2), owner],
            device_id={"blk": target},
        )

    def load_copy(part, owner, target, sem):
        first, count = ((0, 1), (1, steps - 1))[part]
        return pltpu.make_async_remote_copy(
            src_ref=loads.at[owner, pl.ds(first, count)],
            dst_ref=loads.at[owner, pl.ds(first, count)],
            send_sem=sem,
            recv_sem=frecv_sem.at[part, owner],
            device_id={"blk": target},
        )

    def place_out(step, action):
        if cores == 2:
            getattr(place_copy(step, me, twin, send_sem.at[twin]), action)()

        @pl.loop(1, chips)
        def _(order):
            to = peer(order)
            getattr(place_copy(step, me, to, send_sem.at[to]), action)()

    def load_out(part, action):
        if cores == 2:
            getattr(load_copy(part, me, twin, fsend_sem.at[part, twin]), action)()

        @pl.loop(1, chips)
        def _(order):
            to = peer(order)
            getattr(load_copy(part, me, to, fsend_sem.at[part, to]), action)()

    def table_copy(owner, target):
        return pltpu.make_async_remote_copy(
            src_ref=table,
            dst_ref=tables.at[owner],
            send_sem=tsend_sem.at[target],
            recv_sem=trecv_sem.at[owner],
            device_id={"blk": target},
        )

    loads[me] = force_ref[...]
    places[0, me] = pos_ref[...] * 0.5
    pl.semaphore_wait(barrier, n - 1)

    place_out(0, "start")
    load_out(0, "start")
    if steps > 1:
        load_out(1, "start")

    @pl.loop(0, steps)
    def _(step):
        mine = places[step, me]
        padded = jnp.concatenate([mine, jnp.zeros((5, width), jnp.float32)], axis=0)
        turned = jnp.transpose(padded)
        for comp in range(3):
            cols[comp] = jnp.broadcast_to(turned[:, comp : comp + 1], (width, LANES))
            acc[comp] = jnp.zeros((width, LANES), jnp.float32)

        @pl.loop(0, n)
        def _(index):
            if cores == 2:
                direct = jnp.logical_or(
                    index == 0, jnp.logical_and(index % 2 == 1, index < n - 1)
                )
                order = jnp.where(
                    direct,
                    (index + 1) // 2,
                    jnp.where(index == n - 1, chips - 1, (index - 2) // 2),
                )
                side = jnp.where(direct, core, 1 - core)
                source = chip_at(order) * cores + side
                passing = jnp.logical_and(direct, index > 0)
            else:
                source = peer(index)
                passing = None

            @pl.when(index > 0)
            def _():
                place_copy(step, source, source, send_sem.at[source]).wait_recv()

            if passing is not None:

                @pl.when(passing)
                def _():
                    place_copy(step, source, twin, pass_sem.at[0, source]).start()

            for part in range(min(2, steps)):

                @pl.when(jnp.logical_and(index > 0, step == part))
                def _():
                    load_copy(part, source, source, fsend_sem.at[part, source]).wait_recv()

                if passing is not None:

                    @pl.when(jnp.logical_and(passing, step == part))
                    def _():
                        load_copy(part, source, twin, pass_sem.at[part + 1, source]).start()

            @pl.loop(0, width // ROWS)
            def _(chunk):
                rows = pl.ds(pl.multiple_of(chunk * ROWS, ROWS), ROWS)
                target = [cols[comp, rows, :] for comp in range(3)]
                sums = [acc[comp, rows, :] for comp in range(3)]
                for tile in range(tiles):
                    lanes = pl.ds(tile * LANES, LANES)
                    sep = [
                        target[comp] - places[step, source, pl.ds(comp, 1), lanes]
                        for comp in range(3)
                    ]
                    load = [
                        loads[source, step, pl.ds(comp, 1), lanes] for comp in range(3)
                    ]
                    dist_sq = sep[0] * sep[0] + sep[1] * sep[1] + sep[2] * sep[2]
                    dist_sq = jnp.maximum(dist_sq, 1e-30)
                    inv = lax.rsqrt(dist_sq)
                    cut = jnp.minimum(inv, 1.0)
                    cut_sq = cut * cut
                    near = jnp.maximum(1.0 - dist_sq * inv, 0.0)
                    iso = cut * (6.0 + cut_sq) + 9.0 * near
                    rest = 1.0 - cut_sq
                    along = inv - cut * (rest * rest)
                    push = along * (
                        sep[0] * (3.0 * load[0])
                        + sep[1] * (3.0 * load[1])
                        + sep[2] * (3.0 * load[2])
                    )
                    for comp in range(3):
                        sums[comp] = sums[comp] + (iso * load[comp] + push * sep[comp])
                for comp in range(3):
                    acc[comp, rows, :] = sums[comp]

        vel = jnp.concatenate(
            [lane_sums(acc[comp])[0:1] for comp in range(3)], axis=0
        ) * (1.0 / 16.0)

        place_out(step, "wait_send")
        if cores == 2:

            @pl.loop(1, chips)
            def _(order):
                source = peer(order)
                place_copy(step, source, twin, pass_sem.at[0, source]).wait_send()

        fresh = mine + (0.5 * TIME_STEP) * vel + 0.5 * kick_ref[step]
        out_vel[...] = vel

        @pl.when(step < steps - 1)
        def _():
            places[step + 1, me] = fresh

            place_out(step + 1, "start")

        @pl.when(step == steps - 1)
        def _():
            out_pos[...] = 2.0 * fresh

    for part in range(min(2, steps)):
        load_out(part, "wait_send")
        if cores == 2:

            @pl.loop(1, chips)
            def _(order):
                source = peer(order)
                load_copy(part, source, twin, pass_sem.at[part + 1, source]).wait_send()

    get_hv.wait()
    get_ho.wait()
    vel = out_vel[...]
    moved = out_pos[...] - pos_ref[...]
    dot = jnp.zeros((frames, LANES), jnp.float32)
    square = jnp.zeros((frames, LANES), jnp.float32)
    for comp in range(3):
        for tile in range(tiles):
            lanes = slice(tile * LANES, (tile + 1) * LANES)
            dot = dot + vel[comp : comp + 1, lanes] * hv[comp, :, lanes]
            gap = moved[comp : comp + 1, lanes] - ho[comp, :, lanes]
            square = square + gap * gap
    table[...] = jnp.concatenate([lane_sums(dot)[0:1], lane_sums(square)[0:1]], axis=0)

    @pl.loop(1, n)
    def _(index):
        table_copy(me, partner(index)).start()

    onehot = (
        lax.broadcasted_iota(jnp.int32, (frames, lag_ref.shape[1]), 0) == lag_ref[...]
    ).astype(jnp.bfloat16)
    tables[me] = table[...]

    @pl.loop(1, n)
    def _(index):
        table_copy(partner(index), partner(index)).wait_recv()

    whole = tables[0]
    for index in range(1, n):
        whole = whole + tables[index]
    whole = jnp.concatenate([whole, jnp.zeros((6, frames), jnp.float32)], axis=0)
    stat = None
    for piece in pieces(whole):
        term = jnp.dot(piece, onehot, preferred_element_type=jnp.float32)
        stat = term if stat is None else stat + term
    out_stat[...] = stat[0:2] / jnp.float32(width * n)

    @pl.loop(1, n)
    def _(index):
        table_copy(me, partner(index)).wait_send()


def local(n, positions, forces, random_kicks, history_velocity, history_offset, lag_index):
    steps = forces.shape[0]
    width = positions.shape[1]
    frames = history_velocity.shape[0]
    lags = lag_index.shape[0]
    vmem = pl.BlockSpec(memory_space=pltpu.VMEM)
    hbm = pl.BlockSpec(memory_space=pl.ANY)
    return pl.pallas_call(
        functools.partial(kernel, n, steps),
        out_shape=(
            jax.ShapeDtypeStruct((3, width), jnp.float32),
            jax.ShapeDtypeStruct((3, width), jnp.float32),
            jax.ShapeDtypeStruct((2, lags), jnp.float32),
        ),
        in_specs=[vmem, vmem, vmem, hbm, hbm, vmem],
        out_specs=(vmem, vmem, vmem),
        scratch_shapes=[
            pltpu.VMEM((steps, n, 3, width), jnp.float32),
            pltpu.VMEM((n, steps, 3, width), jnp.float32),
            pltpu.VMEM((3, width, LANES), jnp.float32),
            pltpu.VMEM((3, width, LANES), jnp.float32),
            pltpu.VMEM((3, frames, width), jnp.float32),
            pltpu.VMEM((3, frames, width), jnp.float32),
            pltpu.VMEM((2, frames), jnp.float32),
            pltpu.VMEM((n, 2, frames), jnp.float32),
            pltpu.SemaphoreType.DMA((n,)),
            pltpu.SemaphoreType.DMA((2, n)),
            pltpu.SemaphoreType.DMA((3, n)),
            pltpu.SemaphoreType.DMA((2, n)),
            pltpu.SemaphoreType.DMA((2, n)),
            pltpu.SemaphoreType.DMA((n,)),
            pltpu.SemaphoreType.DMA((n,)),
            pltpu.SemaphoreType.DMA((2,)),
        ],
        compiler_params=pltpu.CompilerParams(collective_id=0, has_side_effects=True),
    )(
        positions,
        forces,
        random_kicks,
        history_velocity.transpose(1, 0, 2),
        history_offset.transpose(1, 0, 2),
        lag_index.reshape(1, lags),
    )


def solution(mesh):
    return jax.shard_map(
        functools.partial(local, mesh.shape["blk"]),
        mesh=mesh,
        in_specs=(
            P(None, ("rep", "blk")),
            P(None, None, ("rep", "blk")),
            P(None, None, ("rep", "blk")),
            P(None, None, ("rep", "blk")),
            P(None, None, ("rep", "blk")),
            P(("rep", "blk")),
        ),
        out_specs=(P(None, ("rep", "blk")), P(None, ("rep", "blk")), P(None, ("rep", "blk"))),
        check_vma=False,
    )
```
